32 devices in a mesh: grp: 2 (over y), mode: 8 (over z, x), node: 2 (over core).
Axes of the slice: x: 2, y: 2, z: 4, core: 2. Of those that a mesh axis runs over, the one named last changes fastest.
Arguments:
- mode_basis: float32 [4096, 4096], P('mode', 'node'), may hold values from -6 to 6
- mode_scales: float32 [4096], P('mode'), may hold values from 0.003 to 0.02
- mean_log: float32 [4096], P(('node', 'mode')), may hold values from -0.5 to 0.5
- sample_seeds: int32 [4096], P('grp'), parts along dimension 0, may hold values from 0 to 1073741823
Outputs:
- modulus: float32 [4096, 4096], P(('node', 'mode'), 'grp'), parts along dimension 1
- sample_means: float32 [4096], P('grp'), parts along dimension 0
The draws below stay inside these ranges and needn't reach their ends.
There are 2 independent parts, one for each index of `grp`. The reference program is written for one: setup_inputs(seed, part) draws one part's arguments, and reference() takes and returns one part's arrays. A program takes and returns all parts, laid end to end along the dimension named above; an argument that names none is the same for every part. Nothing has to cross between parts.
All inputs are finite; a program needn't handle non-finite values.
Results may differ from the reference program's by a relative error of at most 0.00005.
Values sent between devices are 32-bit elements; how exact they have to be, the bound alone decides.
A program may use at most 64 MiB of HBM per device.

```python
import math
import jax
import jax.numpy as jnp
from jax import lax

MODES = 4096
SAMPLES = 2048
NODES = 4096


def plant(entries, own_key, smallest, top_value):
    spot = [jax.random.randint(jax.random.fold_in(own_key, axis), (), 0, length) for axis, length in enumerate(entries.shape)]
    widest = entries.shape.index(max(entries.shape))
    neighbour = spot[:widest] + [(spot[widest] + 1) % entries.shape[widest]] + spot[widest + 1:]
    return entries.at[tuple(spot)].set(smallest).at[tuple(neighbour)].set(top_value)


def with_spikes(array, own_key, source, target, blocks, factor):
    owner, partner = [(jnp.arange(array.shape[axis_at]) // (array.shape[axis_at] // blocks)).reshape([-1 if axis == axis_at else 1 for axis in range(array.ndim)]) for axis_at in (source, target)]
    chosen = jax.random.permutation(own_key, blocks)[partner]
    strong = (owner == chosen) | (owner == (partner + blocks // 2) % blocks)
    return jnp.where(strong, factor * array, array)


def level_of(stream_key, dims, split, low, high):
    loudness, own = 1.0, jax.random.fold_in(stream_key, 6)
    for axis_at, shards_of in split:
        draws = jnp.exp(jax.random.uniform(jax.random.fold_in(own, axis_at), (shards_of,), jnp.float32, low / len(split), high / len(split)))
        loudness = loudness * jnp.repeat(draws, dims[axis_at] // shards_of).reshape([-1 if axis == axis_at else 1 for axis in range(len(dims))])
    return loudness


def bell_draw_with(rng, shape, spread, reach, pieces, heavy, kind=jnp.bfloat16):
    entries = spread * jax.random.normal(rng, shape, jnp.float32)
    if pieces:
        entries = entries * level_of(rng, shape, pieces, -0.22, 0.18)
    return jnp.clip(with_spikes(entries, jax.random.fold_in(rng, 3), *heavy), -reach, reach).astype(kind)


def setup_inputs(seed: int = 0, part: int = 0) -> dict:
    key_of = jax.random.split(jax.random.key(seed), 5)
    own_keys = jax.random.split(jax.random.fold_in(key_of[4], part), 5)
    return {
        "mode_basis": bell_draw_with(key_of[0], (MODES, NODES), 1.0, 6.0, ((0, 8), (1, 2)), (0, 1, 8, 2.0), jnp.float32),
        "mode_scales": jnp.clip(jnp.exp(math.log(0.02) - 1.89712 * jax.random.uniform(key_of[1], (MODES,), jnp.float32) ** level_of(key_of[1], (MODES,), ((0, 8),), -0.2, 0.2)), 0.003, 0.02),
        "mean_log": jnp.clip(jax.random.uniform(key_of[2], (NODES,), jnp.float32, -0.5, 0.5) * level_of(key_of[2], (NODES,), ((0, 16),), -0.4, 0.0), -0.5, 0.5),
        "sample_seeds": plant(jax.random.randint(own_keys[3], (SAMPLES,), 0, 1073741824), jax.random.fold_in(own_keys[3], 1), 0, 1073741823).astype(jnp.int32),
    }


def scramble(seed_words, counter_words):
    mixed_word = seed_words * -1640531527 + counter_words * 668265261
    mixed_word = mixed_word ^ mixed_word >> 15 & 131071
    mixed_word = mixed_word * -2048144789
    mixed_word = mixed_word ^ mixed_word >> 13 & 524287
    mixed_word = mixed_word * -1028477387
    mixed_word = mixed_word ^ mixed_word >> 16 & 65535
    return mixed_word

def normals(sample_seeds, mode_start, mode_count):
    mode_ids = mode_start + jnp.arange(mode_count, dtype=jnp.int32)
    seed_words = sample_seeds.astype(jnp.int32)[None, :]
    counter_words = (2 * mode_ids).astype(jnp.int32)[:, None]
    first_word = scramble(seed_words, counter_words)
    second_word = scramble(seed_words, counter_words + 1)
    first_unit = ((first_word & 16777215).astype(jnp.float32) + 0.5) * (1.0 / 16777216.0)
    second_unit = ((second_word & 16777215).astype(jnp.float32) + 0.5) * (1.0 / 16777216.0)
    radius = jnp.sqrt(-2.0 * jnp.log(first_unit))
    return radius * jnp.cos(2.0 * math.pi * second_unit)

def reference(mode_basis, mode_scales, mean_log, sample_seeds):
    scaled = mode_scales[:, None] * mode_basis
    coeffs = normals(sample_seeds, 0, MODES)
    summed = lax.dot_general(scaled, coeffs, (((0,), (0,)), ((), ())), precision=lax.Precision.HIGHEST, preferred_element_type=jnp.float32)
    modulus = jnp.exp(mean_log[:, None] + summed)
    sample_means = lax.optimization_barrier(jnp.sum(modulus, axis=0)) / NODES
    return (modulus, sample_means)
```

```python
import functools
import math

import jax
import jax.numpy as jnp
import numpy as np
from jax import lax
from jax.experimental import pallas as pl
from jax.experimental.pallas import tpu as pltpu
from jax.sharding import PartitionSpec as P

MESH = pl.DeviceIdType.MESH


def sine_series():
    points = 0.25 * np.cos((np.arange(200) + 0.5) * np.pi / 400)
    powers = points[:, None] ** np.arange(0, 11, 2)[None, :]
    values = np.sin(2 * np.pi * points) / points
    return [float(c) for c in np.linalg.lstsq(powers, values, rcond=None)[0]]


SINE = sine_series()


def scramble(word):
    word = word ^ lax.shift_right_logical(word, jnp.int32(15))
    word = word * jnp.int32(-2048144789)
    word = word ^ lax.shift_right_logical(word, jnp.int32(13))
    word = word * jnp.int32(-1028477387)
    return word ^ lax.shift_right_logical(word, jnp.int32(16))


def normals(seed_terms, counter_terms):
    start_word = seed_terms + counter_terms
    first_word = scramble(start_word) & jnp.int32(16777215)
    second_word = scramble(start_word + jnp.int32(668265261)) & jnp.int32(16777215)
    first_unit = (first_word.astype(jnp.float32) + 0.5) * (1.0 / 16777216.0)
    square = -2.0 * jnp.log(first_unit)
    radius = square * lax.rsqrt(jnp.maximum(square, 1e-30))
    folded = jnp.abs(second_word.astype(jnp.float32) - 8388607.5) - 4194304.0
    turn = folded * (1.0 / 16777216.0)
    turn2 = turn * turn
    series = jnp.full_like(turn, SINE[-1])
    for coefficient in SINE[-2::-1]:
        series = series * turn2 + coefficient
    return (radius * turn) * series


def split(values):
    high = values.astype(jnp.bfloat16)
    return high, (values - high.astype(jnp.float32)).astype(jnp.bfloat16)


def kernel(n, basis, scales, mean, seeds, modulus, means, gathered, scale_all, mean_all, coef_hi, coef_lo, lhs_hi, lhs_lo,
           total, staged, parts, halves, net_send, net_recv, row_send, row_recv, core_send, core_recv,
           scale_send, scale_recv, part_send, part_recv, mean_sems, own_sem, out_sems, half_sems):
    g, me, c = lax.axis_index("grp"), lax.axis_index("mode"), lax.axis_index("node")
    _, _, _, half, wide = gathered.shape
    rows = 2 * half
    samples = coef_hi.shape[-1]
    across, sibling = (1 - g, me, c), (g, me, 1 - c)

    def to(step):
        return lax.rem(me + step, n)

    def source(step):
        return lax.rem(me + n - step, n)

    barrier = pltpu.get_barrier_semaphore()

    @pl.loop(1, n)
    def _(step):
        pl.semaphore_signal(barrier, inc=1, device_id=(g, to(step), c), device_id_type=MESH)

    pl.semaphore_signal(barrier, inc=1, device_id=across, device_id_type=MESH)
    pl.semaphore_signal(barrier, inc=1, device_id=sibling, device_id_type=MESH)

    own_scale = scale_all.at[me]
    own_mean = mean_all.at[c]
    own_scale[...] = scales[...]
    own_mean[...] = mean[...]
    own_columns = pl.ds(pl.multiple_of(me * wide, 128), wide)
    own = [
        pltpu.make_async_copy(basis.at[pl.ds(h * half, half), own_columns], gathered.at[c, me, h], own_sem.at[h])
        for h in range(2)
    ]
    for copy in own:
        copy.start()
    pl.semaphore_wait(barrier, n + 1)

    def net(step, owner):
        peer = to(step)
        return pltpu.make_async_remote_copy(
            src_ref=basis.at[pl.ds(pl.multiple_of(g * half, 8), half), pl.ds(pl.multiple_of(peer * wide, 128), wide)],
            dst_ref=gathered.at[c, owner, g],
            send_sem=net_send.at[step], recv_sem=net_recv.at[step], device_id=(g, peer, c), device_id_type=MESH)

    def scale_copy(step, owner):
        return pltpu.make_async_remote_copy(
            src_ref=scales, dst_ref=scale_all.at[owner],
            send_sem=scale_send.at[step], recv_sem=scale_recv.at[step], device_id=(g, to(step), c), device_id_type=MESH)

    def row_copy(step, owner, h):
        block = gathered.at[c, owner, h]
        return pltpu.make_async_remote_copy(
            src_ref=block, dst_ref=block,
            send_sem=row_send.at[step], recv_sem=row_recv.at[step], device_id=across, device_id_type=MESH)

    def core_copy(step, owner, h, side, which):
        block = gathered.at[side, owner, h]
        return pltpu.make_async_remote_copy(
            src_ref=block, dst_ref=block,
            send_sem=core_send.at[which, step], recv_sem=core_recv.at[which, step],
            device_id=sibling, device_id_type=MESH)

    def part_copy(step, owner):
        return pltpu.make_async_remote_copy(
            src_ref=parts.at[me], dst_ref=parts.at[owner],
            send_sem=part_send.at[step], recv_sem=part_recv.at[step], device_id=(g, to(step), c), device_id_type=MESH)

    mean_copy = lambda side: pltpu.make_async_remote_copy(
        src_ref=mean, dst_ref=mean_all.at[side], send_sem=mean_sems.at[0], recv_sem=mean_sems.at[1],
        device_id=sibling, device_id_type=MESH)

    @pl.loop(1, n)
    def _(step):
        net(step, me).start()

    @pl.loop(1, n)
    def _(step):
        scale_copy(step, me).start()

    mean_copy(c).start()
    for copy in own:
        copy.wait()
    core_copy(0, me, g, c, 0).start()
    core_copy(0, me, 1 - g, c, 1).start()

    seed_terms = seeds[:, pl.ds(pl.multiple_of(c * samples, 128), samples)] * jnp.int32(-1640531527)
    lanes = min(512, samples)

    def draw(owner):
        @pl.loop(0, rows // 16)
        def _(tile):
            first = owner * rows + tile * 16
            ids = lax.broadcasted_iota(jnp.int32, (16, lanes), 0) + first
            counters = ids * jnp.int32(2 * 668265261 - 2**32 if 2 * 668265261 >= 2**31 else 2 * 668265261)
            for start in range(0, samples, lanes):
                high, low = split(normals(seed_terms[:, start:start + lanes], counters))
                here = pl.ds(pl.multiple_of(tile * 16, 16), 16)
                coef_hi[owner, here, start:start + lanes] = high
                coef_lo[owner, here, start:start + lanes] = low

    def multiply(step, owner, first):
        core_copy(step, owner, g, 1 - c, 0).wait_recv()
        core_copy(step, owner, 1 - g, 1 - c, 1).wait_recv()
        scale_row = scale_all[owner]
        for side in range(2):
            block = gathered[side, owner].reshape(rows, wide)
            high, low = split(block.T * scale_row)
            lhs_hi[side * wide:(side + 1) * wide, :] = high
            lhs_lo[side * wide:(side + 1) * wide, :] = low
        columns = min(256, samples)

        @pl.loop(0, samples // columns)
        def _(tile):
            here = pl.ds(pl.multiple_of(tile * columns, 128), columns)
            right_hi, right_lo = coef_hi[owner, :, here], coef_lo[owner, :, here]
            dot = functools.partial(jnp.dot, preferred_element_type=jnp.float32)
            product = dot(lhs_hi[...], right_hi) + dot(lhs_lo[...], right_hi) + dot(lhs_hi[...], right_lo)
            if first:
                total[:, here] = product
            else:
                total[:, here] += product

    draw(me)

    def arrive(step):
        owner = source(step)
        net(step, owner).wait_recv()
        row_copy(step, owner, g).start()
        core_copy(step, owner, g, c, 0).start()
        draw(owner)
        row_copy(step, owner, 1 - g).wait_recv()
        core_copy(step, owner, 1 - g, c, 1).start()

    arrive(1)
    multiply(0, me, True)

    @pl.loop(2, n)
    def _(step):
        arrive(step)
        scale_copy(step - 1, source(step - 1)).wait_recv()
        multiply(step - 1, source(step - 1), False)

    scale_copy(n - 1, source(n - 1)).wait_recv()
    multiply(n - 1, source(n - 1), False)
    mean_copy(1 - c).wait_recv()

    sums = jnp.zeros((1, samples), jnp.float32)
    for side in range(2):
        shift = jnp.broadcast_to(mean_all[side], (8, wide)).T[:, :1]
        values = jnp.exp(total[side * wide:(side + 1) * wide, :] + shift)
        staged[side] = values
        sums = sums + jnp.sum(values, axis=0, keepdims=True)
    parts[me] = sums
    out_columns = modulus.at[:, pl.ds(pl.multiple_of(c * samples, 128), samples)]
    other_columns = modulus.at[:, pl.ds(pl.multiple_of((1 - c) * samples, 128), samples)]
    local_out = pltpu.make_async_copy(staged.at[c], out_columns, out_sems.at[0])
    send_out = lambda landing: pltpu.make_async_remote_copy(
        src_ref=staged.at[1 - c], dst_ref=landing, send_sem=out_sems.at[1], recv_sem=out_sems.at[2],
        device_id=sibling, device_id_type=MESH)

    @pl.loop(1, n)
    def _(step):
        part_copy(step, me).start()

    send_out(out_columns).start()
    local_out.start()

    @pl.loop(1, n)
    def _(step):
        part_copy(step, source(step)).wait_recv()

    summed = jnp.zeros((1, samples), jnp.float32)
    for m in range(n):
        summed = summed + parts[m]
    halves[c] = summed / (n * 2 * wide)
    half_copy = lambda side: pltpu.make_async_remote_copy(
        src_ref=halves.at[c], dst_ref=halves.at[side], send_sem=half_sems.at[0], recv_sem=half_sems.at[1],
        device_id=sibling, device_id_type=MESH)
    half_copy(c).start()

    mean_copy(c).wait_send()
    core_copy(0, me, g, c, 0).wait_send()
    core_copy(0, me, 1 - g, c, 1).wait_send()

    @pl.loop(1, n)
    def _(step):
        owner = source(step)
        net(step, me).wait_send()
        scale_copy(step, me).wait_send()
        part_copy(step, me).wait_send()
        row_copy(step, owner, g).wait_send()
        core_copy(step, owner, g, c, 0).wait_send()
        core_copy(step, owner, 1 - g, c, 1).wait_send()

    half_copy(1 - c).wait_recv()
    half_copy(c).wait_send()
    means[:, 0:samples] = halves[0]
    means[:, samples:2 * samples] = halves[1]
    local_out.wait()
    send_out(other_columns).wait_recv()
    send_out(out_columns).wait_send()


def on_device(mode_basis, mode_scales, mean_log, sample_seeds):
    n = lax.axis_size("mode")
    rows, wide, all_samples = mode_scales.shape[0], mean_log.shape[0], sample_seeds.shape[0]
    half, samples = rows // 2, all_samples // 2
    vmem = pl.BlockSpec(memory_space=pltpu.VMEM)
    anywhere = pl.BlockSpec(memory_space=pl.ANY)
    dma = pltpu.SemaphoreType.DMA
    modulus, means = pl.pallas_call(
        functools.partial(kernel, n),
        out_shape=(
            jax.ShapeDtypeStruct((wide, all_samples), jnp.float32),
            jax.ShapeDtypeStruct((1, all_samples), jnp.float32),
        ),
        in_specs=[anywhere, vmem, vmem, vmem],
        out_specs=(anywhere, vmem),
        scratch_shapes=[
            pltpu.VMEM((2, n, 2, half, wide), jnp.float32),
            pltpu.VMEM((n, 1, rows), jnp.float32),
            pltpu.VMEM((2, 1, wide), jnp.float32),
            pltpu.VMEM((n, rows, samples), jnp.bfloat16),
            pltpu.VMEM((n, rows, samples), jnp.bfloat16),
            pltpu.VMEM((2 * wide, rows), jnp.bfloat16),
            pltpu.VMEM((2 * wide, rows), jnp.bfloat16),
            pltpu.VMEM((2 * wide, samples), jnp.float32),
            pltpu.VMEM((2, wide, samples), jnp.float32),
            pltpu.VMEM((n, 1, samples), jnp.float32),
            pltpu.VMEM((2, 1, samples), jnp.float32),
            dma((n,)), dma((n,)), dma((n,)), dma((n,)), dma((2, n)), dma((2, n)),
            dma((n,)), dma((n,)), dma((n,)), dma((n,)), dma((2,)), dma((2,)), dma((3,)), dma((2,)),
        ],
        compiler_params=pltpu.CompilerParams(
            collective_id=0, has_side_effects=True, vmem_limit_bytes=60 * 1024 * 1024
        ),
    )(mode_basis, mode_scales[None, :], mean_log[None, :], sample_seeds[None, :])
    return modulus, means[0]


def solution(mesh):
    return jax.shard_map(
        on_device,
        mesh=mesh,
        in_specs=(P("mode", "node"), P("mode"), P(("node", "mode")), P("grp")),
        out_specs=(P(("node", "mode"), "grp"), P("grp")),
        check_vma=False,
    )
```

```python
import functools
import math

import jax
import jax.numpy as jnp
import numpy as np
from jax import lax
from jax.experimental import pallas as pl
from jax.experimental.pallas import tpu as pltpu
from jax.sharding import PartitionSpec as P

MESH = pl.DeviceIdType.MESH


def sine_series():
    points = 0.25 * np.cos((np.arange(200) + 0.5) * np.pi / 400)
    powers = points[:, None] ** np.arange(0, 11, 2)[None, :]
    values = np.sin(2 * np.pi * points) / points
    return [float(c) for c in np.linalg.lstsq(powers, values, rcond=None)[0]]


SINE = sine_series()


def scramble(word):
    word = word ^ lax.shift_right_logical(word, jnp.int32(15))
    word = word * jnp.int32(-2048144789)
    word = word ^ lax.shift_right_logical(word, jnp.int32(13))
    word = word * jnp.int32(-1028477387)
    return word ^ lax.shift_right_logical(word, jnp.int32(16))


def normals(seed_terms, counter_terms):
    start_word = seed_terms + counter_terms
    first_word = scramble(start_word) & jnp.int32(16777215)
    second_word = scramble(start_word + jnp.int32(668265261)) & jnp.int32(16777215)
    first_unit = (first_word.astype(jnp.float32) + 0.5) * (1.0 / 16777216.0)
    square = -2.0 * jnp.log(first_unit)
    radius = square * lax.rsqrt(jnp.maximum(square, 1e-30))
    folded = jnp.abs(second_word.astype(jnp.float32) - 8388607.5) - 4194304.0
    turn = folded * (1.0 / 16777216.0)
    turn2 = turn * turn
    series = jnp.full_like(turn, SINE[-1])
    for coefficient in SINE[-2::-1]:
        series = series * turn2 + coefficient
    return (radius * turn) * series


def split(values):
    high = values.astype(jnp.bfloat16)
    return high, (values - high.astype(jnp.float32)).astype(jnp.bfloat16)


def kernel(n, basis, scales, mean, seeds, modulus, means, gathered, scale_all, mean_all, coefs, lhs,
           total, staged, parts, halves, net_send, net_recv, row_send, row_recv, core_send, core_recv,
           scale_send, scale_recv, part_send, part_recv, mean_sems, own_sem, out_sems, half_sems):
    g, me, c = lax.axis_index("grp"), lax.axis_index("mode"), lax.axis_index("node")
    _, _, pieces, piece, wide = gathered.shape
    rows = pieces * piece
    mine, theirs = [[side * 2 + p for p in range(2)] for side in (g, 1 - g)]
    samples = coefs.shape[-1]
    across, sibling = (1 - g, me, c), (g, me, 1 - c)

    def to(step):
        flipped, bit = 0, 1
        while bit < n:
            flipped = flipped + lax.rem(me // bit + step // bit, 2) * bit
            bit *= 2
        return flipped

    near, quarter = n // 2, n // 4

    def far(q):
        return near + lax.rem(q, 2) * quarter + q // 2

    barrier = pltpu.get_barrier_semaphore()

    @pl.loop(1, n)
    def _(step):
        pl.semaphore_signal(barrier, inc=1, device_id=(g, to(step), c), device_id_type=MESH)

    pl.semaphore_signal(barrier, inc=1, device_id=across, device_id_type=MESH)
    pl.semaphore_signal(barrier, inc=1, device_id=sibling, device_id_type=MESH)

    own_scale = scale_all.at[me]
    own_mean = mean_all.at[c]
    own_scale[...] = scales[...]
    own_mean[...] = mean[...]
    own_columns = pl.ds(pl.multiple_of(me * wide, 128), wide)
    own = [
        pltpu.make_async_copy(basis.at[pl.ds(k * piece, piece), own_columns], gathered.at[c, me, k], own_sem.at[k])
        for k in range(pieces)
    ]
    for copy in own:
        copy.start()
    pl.semaphore_wait(barrier, n + 1)

    def net(step, owner, k):
        peer = to(step)
        return pltpu.make_async_remote_copy(
            src_ref=basis.at[pl.ds(pl.multiple_of(k * piece, 8), piece), pl.ds(pl.multiple_of(peer * wide, 128), wide)],
            dst_ref=gathered.at[c, owner, k],
            send_sem=net_send.at[k, step], recv_sem=net_recv.at[k, step], device_id=(g, peer, c), device_id_type=MESH)

    def scale_copy(step, owner):
        return pltpu.make_async_remote_copy(
            src_ref=scales, dst_ref=scale_all.at[owner],
            send_sem=scale_send.at[step], recv_sem=scale_recv.at[step], device_id=(g, to(step), c), device_id_type=MESH)

    def row_copy(step, owner, k, p):
        block = gathered.at[c, owner, k]
        return pltpu.make_async_remote_copy(
            src_ref=block, dst_ref=block,
            send_sem=row_send.at[p, step], recv_sem=row_recv.at[p, step], device_id=across, device_id_type=MESH)

    def core_copy(step, owner, k, side):
        block = gathered.at[side, owner, k]
        return pltpu.make_async_remote_copy(
            src_ref=block, dst_ref=block,
            send_sem=core_send.at[k, step], recv_sem=core_recv.at[k, step],
            device_id=sibling, device_id_type=MESH)

    def part_copy(step, owner):
        return pltpu.make_async_remote_copy(
            src_ref=parts.at[me], dst_ref=parts.at[owner],
            send_sem=part_send.at[step], recv_sem=part_recv.at[step], device_id=(g, to(step), c), device_id_type=MESH)

    mean_copy = lambda side: pltpu.make_async_remote_copy(
        src_ref=mean, dst_ref=mean_all.at[side], send_sem=mean_sems.at[0], recv_sem=mean_sems.at[1],
        device_id=sibling, device_id_type=MESH)

    @pl.loop(1, n)
    def _(step):
        scale_copy(step, me).start()

    mean_copy(c).start()

    @pl.loop(1, quarter)
    def _(step):
        for k in range(pieces):
            net(step, me, k).start()

    @pl.loop(quarter, near)
    def _(step):
        for k in mine:
            net(step, me, k).start()

    @pl.loop(0, near)
    def _(q):
        for k in mine:
            net(far(q), me, k).start()

    for copy in own:
        copy.wait()
    for k in range(pieces):
        core_copy(0, me, k, c).start()

    seed_terms = seeds[:, pl.ds(pl.multiple_of(c * samples, 128), samples)] * jnp.int32(-1640531527)
    lanes = min(512, samples)

    def draw(owner):
        @pl.loop(0, rows // 16)
        def _(tile):
            first = owner * rows + tile * 16
            ids = lax.broadcasted_iota(jnp.int32, (16, lanes), 0) + first
            counters = ids * jnp.int32(2 * 668265261 - 2**32 if 2 * 668265261 >= 2**31 else 2 * 668265261)
            for start in range(0, samples, lanes):
                high, low = split(normals(seed_terms[:, start:start + lanes], counters))
                for part, values in enumerate((high, low, high)):
                    here = pl.ds(pl.multiple_of(part * rows + tile * 16, 16), 16)
                    coefs[owner, here, start:start + lanes] = values

    def multiply(step, owner, first):
        for k in range(pieces):
            core_copy(step, owner, k, 1 - c).wait_recv()
        scale_row = scale_all[owner]
        for side in range(2):
            block = gathered[side, owner].reshape(rows, wide)
            high, low = split(block.T * scale_row)
            for part, values in enumerate((high, high, low)):
                lhs[side * wide:(side + 1) * wide, part * rows:(part + 1) * rows] = values
        columns = min(512, samples)

        @pl.loop(0, samples // columns)
        def _(tile):
            here = pl.ds(pl.multiple_of(tile * columns, 128), columns)
            product = jnp.dot(lhs[...], coefs[owner, :, here], preferred_element_type=jnp.float32)
            if first:
                total[:, here] = product
            else:
                total[:, here] += product

    draw(me)

    def forward(step):
        owner = to(step)
        for p, k in enumerate(mine):
            net(step, owner, k).wait_recv()
            row_copy(step, owner, k, p).start()
            core_copy(step, owner, k, c).start()

    def finish(step):
        owner = to(step)
        for p, k in enumerate(theirs):
            row_copy(step, owner, k, p).wait_recv()
            core_copy(step, owner, k, c).start()

    def use(step):
        scale_copy(step, to(step)).wait_recv()
        multiply(step, to(step), False)

    @pl.loop(1, quarter)
    def _(step):
        draw(to(step))

    multiply(0, me, True)

    @pl.loop(0, quarter)
    def _(q):
        draw(to(quarter + q))
        forward(quarter + q)
        draw(to(far(q)))
        draw(to(far(quarter + q)))
        forward(far(q))

    @pl.loop(1, quarter)
    def _(step):
        for k in range(pieces):
            net(step, to(step), k).wait_recv()
            core_copy(step, to(step), k, c).start()

    @pl.loop(quarter, near)
    def _(step):
        finish(step)

    @pl.loop(1, near - quarter // 2)
    def _(step):
        use(step)

    @pl.loop(quarter, near)
    def _(q):
        forward(far(q))

    @pl.loop(0, quarter)
    def _(q):
        finish(far(q))

    @pl.loop(near - quarter // 2, near)
    def _(step):
        use(step)

    @pl.loop(0, quarter)
    def _(q):
        use(far(q))

    @pl.loop(quarter, near)
    def _(q):
        finish(far(q))
        use(far(q))

    mean_copy(1 - c).wait_recv()

    sums = jnp.zeros((1, samples), jnp.float32)
    for side in range(2):
        shift = jnp.broadcast_to(mean_all[side], (8, wide)).T[:, :1]
        values = jnp.exp(total[side * wide:(side + 1) * wide, :] + shift)
        staged[side] = values
        sums = sums + jnp.sum(values, axis=0, keepdims=True)
    parts[me] = sums
    out_columns = modulus.at[:, pl.ds(pl.multiple_of(c * samples, 128), samples)]
    other_columns = modulus.at[:, pl.ds(pl.multiple_of((1 - c) * samples, 128), samples)]
    local_out = pltpu.make_async_copy(staged.at[c], out_columns, out_sems.at[0])
    send_out = lambda landing: pltpu.make_async_remote_copy(
        src_ref=staged.at[1 - c], dst_ref=landing, send_sem=out_sems.at[1], recv_sem=out_sems.at[2],
        device_id=sibling, device_id_type=MESH)

    @pl.loop(1, n)
    def _(step):
        part_copy(step, me).start()

    send_out(out_columns).start()
    local_out.start()

    @pl.loop(1, n)
    def _(step):
        part_copy(step, to(step)).wait_recv()

    summed = jnp.zeros((1, samples), jnp.float32)
    for m in range(n):
        summed = summed + parts[m]
    halves[c] = summed / (n * 2 * wide)
    half_copy = lambda side: pltpu.make_async_remote_copy(
        src_ref=halves.at[c], dst_ref=halves.at[side], send_sem=half_sems.at[0], recv_sem=half_sems.at[1],
        device_id=sibling, device_id_type=MESH)
    half_copy(c).start()

    mean_copy(c).wait_send()
    for k in range(pieces):
        core_copy(0, me, k, c).wait_send()

    @pl.loop(1, n)
    def _(step):
        scale_copy(step, me).wait_send()
        part_copy(step, me).wait_send()
        for k in range(pieces):
            core_copy(step, to(step), k, c).wait_send()
        for k in mine:
            net(step, me, k).wait_send()

    @pl.loop(1, quarter)
    def _(step):
        for k in theirs:
            net(step, me, k).wait_send()

    @pl.loop(quarter, n)
    def _(step):
        for p, k in enumerate(mine):
            row_copy(step, to(step), k, p).wait_send()

    half_copy(1 - c).wait_recv()
    half_copy(c).wait_send()
    means[:, 0:samples] = halves[0]
    means[:, samples:2 * samples] = halves[1]
    local_out.wait()
    send_out(other_columns).wait_recv()
    send_out(out_columns).wait_send()


def on_device(mode_basis, mode_scales, mean_log, sample_seeds):
    n = lax.axis_size("mode")
    rows, wide, all_samples = mode_scales.shape[0], mean_log.shape[0], sample_seeds.shape[0]
    piece, samples = rows // 4, all_samples // 2
    vmem = pl.BlockSpec(memory_space=pltpu.VMEM)
    anywhere = pl.BlockSpec(memory_space=pl.ANY)
    dma = pltpu.SemaphoreType.DMA
    modulus, means = pl.pallas_call(
        functools.partial(kernel, n),
        out_shape=(
            jax.ShapeDtypeStruct((wide, all_samples), jnp.float32),
            jax.ShapeDtypeStruct((1, all_samples), jnp.float32),
        ),
        in_specs=[anywhere, vmem, vmem, vmem],
        out_specs=(anywhere, vmem),
        scratch_shapes=[
            pltpu.VMEM((2, n, 4, piece, wide), jnp.float32),
            pltpu.VMEM((n, 1, rows), jnp.float32),
            pltpu.VMEM((2, 1, wide), jnp.float32),
            pltpu.VMEM((n, 3 * rows, samples), jnp.bfloat16),
            pltpu.VMEM((2 * wide, 3 * rows), jnp.bfloat16),
            pltpu.VMEM((2 * wide, samples), jnp.float32),
            pltpu.VMEM((2, wide, samples), jnp.float32),
            pltpu.VMEM((n, 1, samples), jnp.float32),
            pltpu.VMEM((2, 1, samples), jnp.float32),
            dma((4, n)), dma((4, n)), dma((2, n)), dma((2, n)), dma((4, n)), dma((4, n)),
            dma((n,)), dma((n,)), dma((n,)), dma((n,)), dma((2,)), dma((4,)), dma((3,)), dma((2,)),
        ],
        compiler_params=pltpu.CompilerParams(
            collective_id=0, has_side_effects=True, vmem_limit_bytes=60 * 1024 * 1024
        ),
    )(mode_basis, mode_scales[None, :], mean_log[None, :], sample_seeds[None, :])
    return modulus, means[0]


def solution(mesh):
    return jax.shard_map(
        on_device,
        mesh=mesh,
        in_specs=(P("mode", "node"), P("mode"), P(("node", "mode")), P("grp")),
        out_specs=(P(("node", "mode"), "grp"), P("grp")),
        check_vma=False,
    )
```

```python
import functools
import math

import jax
import jax.numpy as jnp
import numpy as np
from jax import lax
from jax.experimental import pallas as pl
from jax.experimental.pallas import tpu as pltpu
from jax.sharding import PartitionSpec as P

MESH = pl.DeviceIdType.MESH


def sine_series():
    points = 0.25 * np.cos((np.arange(200) + 0.5) * np.pi / 400)
    powers = points[:, None] ** np.arange(0, 11, 2)[None, :]
    values = np.sin(2 * np.pi * points) / points
    return [float(c) for c in np.linalg.lstsq(powers, values, rcond=None)[0]]


SINE = sine_series()


def scramble(word):
    word = word ^ lax.shift_right_logical(word, jnp.int32(15))
    word = word * jnp.int32(-2048144789)
    word = word ^ lax.shift_right_logical(word, jnp.int32(13))
    word = word * jnp.int32(-1028477387)
    return word ^ lax.shift_right_logical(word, jnp.int32(16))


def normals(seed_terms, counter_terms):
    start_word = seed_terms + counter_terms
    first_word = scramble(start_word) & jnp.int32(16777215)
    second_word = scramble(start_word + jnp.int32(668265261)) & jnp.int32(16777215)
    first_unit = (first_word.astype(jnp.float32) + 0.5) * (1.0 / 16777216.0)
    square = -2.0 * jnp.log(first_unit)
    radius = square * lax.rsqrt(jnp.maximum(square, 1e-30))
    folded = jnp.abs(second_word.astype(jnp.float32) - 8388607.5) - 4194304.0
    turn = folded * (1.0 / 16777216.0)
    turn2 = turn * turn
    series = jnp.full_like(turn, SINE[-1])
    for coefficient in SINE[-2::-1]:
        series = series * turn2 + coefficient
    return (radius * turn) * series


def split(values):
    high = values.astype(jnp.bfloat16)
    return high, (values - high.astype(jnp.float32)).astype(jnp.bfloat16)


def kernel(n, basis, scales, mean, seeds, modulus, means, gathered, scale_all, mean_all, coefs, lhs,
           total, staged, parts, halves, net_send, net_recv, row_send, row_recv, core_send, core_recv,
           scale_send, scale_recv, part_send, part_recv, mean_sems, own_sem, out_sems, half_sems):
    g, me, c = lax.axis_index("grp"), lax.axis_index("mode"), lax.axis_index("node")
    _, _, pieces, piece, wide = gathered.shape
    rows = pieces * piece
    mine, theirs = [[side * 2 + p for p in range(2)] for side in (g, 1 - g)]
    samples = coefs.shape[-1]
    across, sibling = (1 - g, me, c), (g, me, 1 - c)

    def to(step):
        flipped, bit = 0, 1
        while bit < n:
            flipped = flipped + lax.rem(me // bit + step // bit, 2) * bit
            bit *= 2
        return flipped

    near, quarter = n // 2, n // 4

    def far(q):
        return near + lax.rem(q, 2) * quarter + q // 2

    barrier = pltpu.get_barrier_semaphore()

    @pl.loop(1, n)
    def _(step):
        pl.semaphore_signal(barrier, inc=1, device_id=(g, to(step), c), device_id_type=MESH)

    pl.semaphore_signal(barrier, inc=1, device_id=across, device_id_type=MESH)
    pl.semaphore_signal(barrier, inc=1, device_id=sibling, device_id_type=MESH)

    own_scale = scale_all.at[me]
    own_mean = mean_all.at[c]
    own_scale[...] = scales[...]
    own_mean[...] = mean[...]
    own_columns = pl.ds(pl.multiple_of(me * wide, 128), wide)
    own = [
        pltpu.make_async_copy(basis.at[pl.ds(k * piece, piece), own_columns], gathered.at[c, me, k], own_sem.at[k])
        for k in range(pieces)
    ]
    for copy in own:
        copy.start()
    pl.semaphore_wait(barrier, n + 1)

    def net(step, owner, k):
        peer = to(step)
        return pltpu.make_async_remote_copy(
            src_ref=basis.at[pl.ds(pl.multiple_of(k * piece, 8), piece), pl.ds(pl.multiple_of(peer * wide, 128), wide)],
            dst_ref=gathered.at[c, owner, k],
            send_sem=net_send.at[k, step], recv_sem=net_recv.at[k, step], device_id=(g, peer, c), device_id_type=MESH)

    def scale_copy(step, owner):
        return pltpu.make_async_remote_copy(
            src_ref=scales, dst_ref=scale_all.at[owner],
            send_sem=scale_send.at[step], recv_sem=scale_recv.at[step], device_id=(g, to(step), c), device_id_type=MESH)

    def row_copy(step, owner, k, p):
        block = gathered.at[c, owner, k]
        return pltpu.make_async_remote_copy(
            src_ref=block, dst_ref=block,
            send_sem=row_send.at[p, step], recv_sem=row_recv.at[p, step], device_id=across, device_id_type=MESH)

    def core_copy(step, owner, k, side):
        block = gathered.at[side, owner, k]
        return pltpu.make_async_remote_copy(
            src_ref=block, dst_ref=block,
            send_sem=core_send.at[k, step], recv_sem=core_recv.at[k, step],
            device_id=sibling, device_id_type=MESH)

    def part_copy(step, owner):
        return pltpu.make_async_remote_copy(
            src_ref=parts.at[me], dst_ref=parts.at[owner],
            send_sem=part_send.at[step], recv_sem=part_recv.at[step], device_id=(g, to(step), c), device_id_type=MESH)

    mean_copy = lambda side: pltpu.make_async_remote_copy(
        src_ref=mean, dst_ref=mean_all.at[side], send_sem=mean_sems.at[0], recv_sem=mean_sems.at[1],
        device_id=sibling, device_id_type=MESH)

    @pl.loop(1, n)
    def _(step):
        scale_copy(step, me).start()

    mean_copy(c).start()

    @pl.loop(1, quarter)
    def _(step):
        for k in range(pieces):
            net(step, me, k).start()

    @pl.loop(quarter, near)
    def _(step):
        for k in mine:
            net(step, me, k).start()

    @pl.loop(0, near)
    def _(q):
        for k in mine:
            net(far(q), me, k).start()

    for copy in own:
        copy.wait()
    for k in range(pieces):
        core_copy(0, me, k, c).start()

    seed_terms = seeds[:, pl.ds(pl.multiple_of(c * samples, 128), samples)] * jnp.int32(-1640531527)
    lanes = min(512, samples)

    def draw(owner):
        @pl.loop(0, rows // 16)
        def _(tile):
            first = owner * rows + tile * 16
            ids = lax.broadcasted_iota(jnp.int32, (16, lanes), 0) + first
            counters = ids * jnp.int32(2 * 668265261 - 2**32 if 2 * 668265261 >= 2**31 else 2 * 668265261)
            for start in range(0, samples, lanes):
                high, low = split(normals(seed_terms[:, start:start + lanes], counters))
                for part, values in enumerate((high, low, high)):
                    here = pl.ds(pl.multiple_of(part * rows + tile * 16, 16), 16)
                    coefs[owner, here, start:start + lanes] = values

    def multiply(step, owner, first):
        for k in range(pieces):
            core_copy(step, owner, k, 1 - c).wait_recv()
        scale_row = scale_all[owner]
        for side in range(2):
            block = gathered[side, owner].reshape(rows, wide)
            high, low = split(block.T * scale_row)
            for part, values in enumerate((high, high, low)):
                lhs[side * wide:(side + 1) * wide, part * rows:(part + 1) * rows] = values
        columns = min(1024, samples)

        @pl.loop(0, samples // columns)
        def _(tile):
            here = pl.ds(pl.multiple_of(tile * columns, 128), columns)
            product = jnp.dot(lhs[...], coefs[owner, :, here], preferred_element_type=jnp.float32)
            if first:
                total[:, here] = product
            else:
                total[:, here] += product

    draw(me)

    def forward(step):
        owner = to(step)
        for p, k in enumerate(mine):
            net(step, owner, k).wait_recv()
            row_copy(step, owner, k, p).start()
            core_copy(step, owner, k, c).start()

    def finish(step):
        owner = to(step)
        for p, k in enumerate(theirs):
            row_copy(step, owner, k, p).wait_recv()
            core_copy(step, owner, k, c).start()

    def use(step):
        scale_copy(step, to(step)).wait_recv()
        multiply(step, to(step), False)

    @pl.loop(1, quarter)
    def _(step):
        draw(to(step))

    multiply(0, me, True)

    @pl.loop(0, quarter)
    def _(q):
        draw(to(quarter + q))
        forward(quarter + q)
        draw(to(far(q)))
        draw(to(far(quarter + q)))
        forward(far(q))

    @pl.loop(1, quarter)
    def _(step):
        for k in range(pieces):
            net(step, to(step), k).wait_recv()
            core_copy(step, to(step), k, c).start()

    @pl.loop(quarter, near)
    def _(step):
        finish(step)

    @pl.loop(1, near - quarter // 2)
    def _(step):
        use(step)

    @pl.loop(quarter, near)
    def _(q):
        forward(far(q))

    @pl.loop(0, quarter)
    def _(q):
        finish(far(q))

    @pl.loop(near - quarter // 2, near)
    def _(step):
        use(step)

    @pl.loop(0, quarter)
    def _(q):
        use(far(q))
        finish(far(quarter + q))

    @pl.loop(quarter, near)
    def _(q):
        use(far(q))

    mean_copy(1 - c).wait_recv()

    sums = jnp.zeros((1, samples), jnp.float32)
    for side in range(2):
        shift = jnp.broadcast_to(mean_all[side], (8, wide)).T[:, :1]
        values = jnp.exp(total[side * wide:(side + 1) * wide, :] + shift)
        staged[side] = values
        sums = sums + jnp.sum(values, axis=0, keepdims=True)
    parts[me] = sums
    out_columns = modulus.at[:, pl.ds(pl.multiple_of(c * samples, 128), samples)]
    other_columns = modulus.at[:, pl.ds(pl.multiple_of((1 - c) * samples, 128), samples)]
    local_out = pltpu.make_async_copy(staged.at[c], out_columns, out_sems.at[0])
    send_out = lambda landing: pltpu.make_async_remote_copy(
        src_ref=staged.at[1 - c], dst_ref=landing, send_sem=out_sems.at[1], recv_sem=out_sems.at[2],
        device_id=sibling, device_id_type=MESH)

    @pl.loop(1, n)
    def _(step):
        part_copy(step, me).start()

    send_out(out_columns).start()
    local_out.start()

    @pl.loop(1, n)
    def _(step):
        part_copy(step, to(step)).wait_recv()

    summed = jnp.zeros((1, samples), jnp.float32)
    for m in range(n):
        summed = summed + parts[m]
    halves[c] = summed / (n * 2 * wide)
    half_copy = lambda side: pltpu.make_async_remote_copy(
        src_ref=halves.at[c], dst_ref=halves.at[side], send_sem=half_sems.at[0], recv_sem=half_sems.at[1],
        device_id=sibling, device_id_type=MESH)
    half_copy(c).start()

    mean_copy(c).wait_send()
    for k in range(pieces):
        core_copy(0, me, k, c).wait_send()

    @pl.loop(1, n)
    def _(step):
        scale_copy(step, me).wait_send()
        part_copy(step, me).wait_send()
        for k in range(pieces):
            core_copy(step, to(step), k, c).wait_send()
        for k in mine:
            net(step, me, k).wait_send()

    @pl.loop(1, quarter)
    def _(step):
        for k in theirs:
            net(step, me, k).wait_send()

    @pl.loop(quarter, n)
    def _(step):
        for p, k in enumerate(mine):
            row_copy(step, to(step), k, p).wait_send()

    half_copy(1 - c).wait_recv()
    half_copy(c).wait_send()
    means[:, 0:samples] = halves[0]
    means[:, samples:2 * samples] = halves[1]
    local_out.wait()
    send_out(other_columns).wait_recv()
    send_out(out_columns).wait_send()


def on_device(mode_basis, mode_scales, mean_log, sample_seeds):
    n = lax.axis_size("mode")
    rows, wide, all_samples = mode_scales.shape[0], mean_log.shape[0], sample_seeds.shape[0]
    piece, samples = rows // 4, all_samples // 2
    vmem = pl.BlockSpec(memory_space=pltpu.VMEM)
    anywhere = pl.BlockSpec(memory_space=pl.ANY)
    dma = pltpu.SemaphoreType.DMA
    modulus, means = pl.pallas_call(
        functools.partial(kernel, n),
        out_shape=(
            jax.ShapeDtypeStruct((wide, all_samples), jnp.float32),
            jax.ShapeDtypeStruct((1, all_samples), jnp.float32),
        ),
        in_specs=[anywhere, vmem, vmem, vmem],
        out_specs=(anywhere, vmem),
        scratch_shapes=[
            pltpu.VMEM((2, n, 4, piece, wide), jnp.float32),
            pltpu.VMEM((n, 1, rows), jnp.float32),
            pltpu.VMEM((2, 1, wide), jnp.float32),
            pltpu.VMEM((n, 3 * rows, samples), jnp.bfloat16),
            pltpu.VMEM((2 * wide, 3 * rows), jnp.bfloat16),
            pltpu.VMEM((2 * wide, samples), jnp.float32),
            pltpu.VMEM((2, wide, samples), jnp.float32),
            pltpu.VMEM((n, 1, samples), jnp.float32),
            pltpu.VMEM((2, 1, samples), jnp.float32),
            dma((4, n)), dma((4, n)), dma((2, n)), dma((2, n)), dma((4, n)), dma((4, n)),
            dma((n,)), dma((n,)), dma((n,)), dma((n,)), dma((2,)), dma((4,)), dma((3,)), dma((2,)),
        ],
        compiler_params=pltpu.CompilerParams(
            collective_id=0, has_side_effects=True, vmem_limit_bytes=60 * 1024 * 1024
        ),
    )(mode_basis, mode_scales[None, :], mean_log[None, :], sample_seeds[None, :])
    return modulus, means[0]


def solution(mesh):
    return jax.shard_map(
        on_device,
        mesh=mesh,
        in_specs=(P("mode", "node"), P("mode"), P(("node", "mode")), P("grp")),
        out_specs=(P(("node", "mode"), "grp"), P("grp")),
        check_vma=False,
    )
```
